32 devices in a mesh: grp: 4 (over y, core), dev: 8 (over z, x).
Axes of the slice: x: 2, y: 2, z: 4, core: 2. Of those that a mesh axis runs over, the one named last changes fastest.
Arguments:
- basis_values: bfloat16 [128, 256, 512], P(('grp', 'dev')), may hold values from -1 to 1
- stored_density_blocks: bfloat16 [64, 128, 128], P('dev'), may hold values from -0.5 to 0.5
- device_request: int32 [32, 8, 8], P(('grp', 'dev')), may hold values from -1 to 7, as said below
- batch_blocks: int32 [128, 16], P(('grp', 'dev')), may hold values from 0 to 63, as said below
- batch_atom: int32 [128], P(('grp', 'dev')), may hold values from 0 to 999
- point_offset: float32 [3, 128, 256], P(None, ('grp', 'dev')), may hold values from -8 to 8
- point_weight: float32 [128, 256], P(('grp', 'dev')), may hold values from 0.02 to 0.5
- exchange_kernel: float32 [128, 256], P(('grp', 'dev')), may hold values from -3 to -0.3
- atom_xyz: float32 [3, 1000], replicated, may hold values from -15 to 15
Outputs:
- response_hamiltonian: bfloat16 [64, 128, 128], P('dev')
- response_density: float32 [128, 256], P(('grp', 'dev'))
- multipoles: float32 [4, 1000], replicated
The draws below stay inside these ranges and needn't reach their ends.
Inputs may be any that keep to these rules, and one draw needn't show every extreme that they name: `device_request`: row d belongs to device d of grp+dev in grp-major order. Each row has exactly 32 entries other than -1, distinct for one owner; in every group one owner is asked for 8 blocks by every device of the group. `batch_blocks`: every entry points to an entry of its device's request row that is not -1.
All inputs are finite; a program needn't handle non-finite values.
Results may differ from the reference program's by a relative error of at most 0.004.
Values may be sent and summed in bfloat16 or wider, within the bound.
A program may use at most 64 MiB of HBM per device.

```python
import math
import jax
import jax.numpy as jnp
from jax import lax

TILE_FUNCTIONS = 128
REL = 4
PTS = 256
BATCH_DEV = 4
OWN_DEV = 8
NEED = 32
ATOMS = 1000
OWNERS = 8
CAP = 8
NBATCH = 128
STORED_BLOCKS = 64


def request_layout(key):
    device_list = NBATCH // BATCH_DEV
    positions = OWNERS * CAP
    hot = jax.random.randint(jax.random.fold_in(key, 11), (device_list // OWNERS,), 0, OWNERS)
    hot_device = jnp.repeat(hot, OWNERS)
    owner_of = jnp.arange(positions, dtype=jnp.int32) // CAP
    noise = jax.random.randint(jax.random.fold_in(key, 12), (device_list, positions), 1, 2 ** 20)
    index = jnp.arange(positions, dtype=jnp.int32)[None, :]
    score = jnp.where(owner_of[None, :] == hot_device[:, None], index, noise * positions + index)
    order = jnp.argsort(score, axis=1).astype(jnp.int32)
    rank = jnp.argsort(order, axis=1)
    live = rank < NEED
    shuffle = jax.random.randint(jax.random.fold_in(key, 13), (device_list, OWNERS, OWN_DEV), 0, 2 ** 20)
    rank_ordered = shuffle * OWN_DEV + jnp.arange(OWN_DEV, dtype=jnp.int32)
    picks = jnp.argsort(rank_ordered, axis=2)[:, :, :CAP].astype(jnp.int32)
    request = jnp.where(live.reshape(device_list, OWNERS, CAP), picks, -1).astype(jnp.int32)
    return (request, order[:, :NEED])


def draw_device_request(key, part):
    return request_layout(key)[0]


def draw_batch_blocks(key, part):
    request, live_positions = request_layout(key)
    device_list = NBATCH // BATCH_DEV
    chosen = jax.random.randint(jax.random.fold_in(key, 14), (device_list, BATCH_DEV * REL * REL), 0, NEED)
    picked = jnp.take_along_axis(live_positions, chosen, axis=1)
    return picked.reshape(NBATCH, REL * REL).astype(jnp.int32)


def with_ends(values, rng, smallest, high):
    index_at = [jax.random.randint(jax.random.fold_in(rng, axis), (), 0, length) for axis, length in enumerate(values.shape)]
    widest = values.shape.index(max(values.shape))
    next_to = index_at[:widest] + [(index_at[widest] + 1) % values.shape[widest]] + index_at[widest + 1:]
    return values.at[tuple(index_at)].set(smallest).at[tuple(next_to)].set(high)


def shard_levels(rng, extent, cuts, smallest, top_value):
    level, own = 1.0, jax.random.fold_in(rng, 6)
    for position, blocks in cuts:
        steps = jnp.exp(jax.random.uniform(jax.random.fold_in(own, position), (blocks,), jnp.float32, smallest / len(cuts), top_value / len(cuts)))
        level = level * jnp.repeat(steps, extent[position] // blocks).reshape([-1 if axis == position else 1 for axis in range(len(extent))])
    return level


def scatter_about(stream_key, dims, deviation, reach, pieces=(), kind=jnp.bfloat16):
    array = deviation * jax.random.normal(stream_key, dims, jnp.float32)
    if pieces:
        array = array * shard_levels(stream_key, dims, pieces, -0.22, 0.18)
    return jnp.clip(array, -reach, reach).astype(kind)


def setup_inputs(seed: int = 0) -> dict:
    keys = jax.random.split(jax.random.key(seed), 10)
    basis_values = scatter_about(keys[0], (NBATCH, PTS, REL * TILE_FUNCTIONS), 0.15, 1.0, ((0, 32),))
    stored_density_blocks = scatter_about(keys[1], (STORED_BLOCKS, TILE_FUNCTIONS, TILE_FUNCTIONS), TILE_FUNCTIONS ** -0.5, 0.5, ((0, 8),))
    device_request = draw_device_request(jax.random.fold_in(keys[9], 71), 0)
    batch_blocks = draw_batch_blocks(jax.random.fold_in(keys[9], 71), 0)
    batch_atom = with_ends(jax.random.randint(keys[4], (NBATCH,), 0, ATOMS), jax.random.fold_in(keys[4], 1), 0, ATOMS - 1).astype(jnp.int32)
    point_offset = scatter_about(keys[5], (3, NBATCH, PTS), 1.5, 8.0, ((1, 32),), jnp.float32)
    point_weight = jnp.clip(jnp.exp(math.log(0.5) - 3.218876 * jax.random.uniform(keys[6], (NBATCH, PTS), jnp.float32) ** shard_levels(keys[6], (NBATCH, PTS), ((0, 32),), -0.2, 0.2)), 0.02, 0.5)
    exchange_kernel = jnp.clip(-3.0 + 2.7 * jax.random.uniform(keys[7], (NBATCH, PTS), jnp.float32) ** shard_levels(keys[7], (NBATCH, PTS), ((0, 32),), -0.2, 0.2), -3.0, -0.3)
    atom_xyz = jnp.clip(jax.random.uniform(keys[8], (3, ATOMS), jnp.float32, -15.0, 15.0), -15.0, 15.0)
    return {"basis_values": basis_values, "stored_density_blocks": stored_density_blocks, "device_request": device_request, "batch_blocks": batch_blocks, "batch_atom": batch_atom, "point_offset": point_offset, "point_weight": point_weight, "exchange_kernel": exchange_kernel, "atom_xyz": atom_xyz}


HIGH = lax.Precision.HIGHEST

def far_field(multipoles, centre, offset, atom_xyz):
    gap = centre[:, None, None] + offset[:, :, None] - atom_xyz[:, None, :]
    inverse = lax.rsqrt(gap[0] * gap[0] + gap[1] * gap[1] + gap[2] * gap[2] + 1.0)
    cube = inverse * inverse * inverse
    dipole = multipoles[1] * gap[0] + multipoles[2] * gap[1] + multipoles[3] * gap[2]
    return lax.optimization_barrier(jnp.sum(multipoles[0] * inverse + dipole * cube, axis=1))

def reference(basis_values, stored_density_blocks, device_request, batch_blocks, batch_atom, point_offset, point_weight, exchange_kernel, atom_xyz):
    device_list, owners, capacity = device_request.shape
    own = stored_density_blocks.shape[0] // owners
    tile = stored_density_blocks.shape[1]
    batches, points, width = basis_values.shape
    rel = width // tile
    per_dev = batches // device_list
    atoms = atom_xyz.shape[1]
    owner_base = (jnp.arange(owners, dtype=jnp.int32) * own)[None, :, None]
    wanted = jnp.where(device_request >= 0, device_request + owner_base, -1).reshape(device_list, owners * capacity)
    batch_home = (jnp.arange(batches, dtype=jnp.int32) // per_dev).astype(jnp.int32)
    batch_slots = jnp.take_along_axis(wanted[batch_home], batch_blocks, axis=1)

    def density_one(args):
        values, slots = args
        blocks = stored_density_blocks[slots].astype(jnp.float32).reshape(rel, rel, tile, tile)
        split = values.astype(jnp.float32).reshape(points, rel, tile)
        left = jnp.einsum('rim,ijmn->rijn', split, blocks)
        return jnp.einsum('rijn,rjn->r', left, split)
    density_field = lax.map(density_one, (basis_values, batch_slots))
    weighted = density_field * point_weight
    parts = jnp.stack([lax.optimization_barrier(jnp.sum(weighted, 1)), lax.optimization_barrier(jnp.sum(weighted * point_offset[0], 1)), lax.optimization_barrier(jnp.sum(weighted * point_offset[1], 1)), lax.optimization_barrier(jnp.sum(weighted * point_offset[2], 1))])
    onehot = (batch_atom[:, None] == jnp.arange(atoms, dtype=jnp.int32)[None, :]).astype(jnp.float32)
    multipoles = jnp.dot(parts, onehot, precision=HIGH)
    centres = jnp.take(atom_xyz, batch_atom, axis=1)

    def potential_one(args):
        centre, offset = args
        return far_field(multipoles, centre, offset, atom_xyz)
    hartree = lax.map(potential_one, (centres.T, jnp.moveaxis(point_offset, 1, 0)))
    xc_part = point_weight * exchange_kernel * density_field
    hartree_part = point_weight * hartree

    def pair_terms(args):
        values, first, second = args
        wide = values.astype(jnp.float32)
        split = wide.reshape(points, rel, tile)
        one = (wide * first[:, None]).astype(jnp.bfloat16).astype(jnp.float32).reshape(points, rel, tile)
        two = (wide * second[:, None]).astype(jnp.bfloat16).astype(jnp.float32).reshape(points, rel, tile)
        return jnp.einsum('rim,rjn->ijmn', one, split) + jnp.einsum('rim,rjn->ijmn', two, split)

    def per_device(total, args):
        values, first, second, positions, requested_row = args
        terms = lax.map(pair_terms, (values, first, second))
        summed = jax.ops.segment_sum(terms.reshape(per_dev * rel * rel, tile * tile), positions.reshape(-1), num_segments=owners * capacity)
        rounded = lax.optimization_barrier(summed.astype(jnp.bfloat16)).astype(jnp.float32)
        target = jnp.where(requested_row >= 0, requested_row, total.shape[0]).astype(jnp.int32)
        return (total.at[target].add(rounded, mode='drop'), None)
    start_total = jnp.zeros((owners * own, tile * tile), jnp.float32)
    total, _ = lax.scan(per_device, start_total, (basis_values.reshape(device_list, per_dev, points, width), xc_part.reshape(device_list, per_dev, points), hartree_part.reshape(device_list, per_dev, points), batch_blocks.reshape(device_list, per_dev, rel * rel), wanted))
    hamiltonian = total.astype(jnp.bfloat16).reshape(owners * own, tile, tile)
    return (hamiltonian, density_field, multipoles)
```

```python
import functools

import jax
import jax.numpy as jnp
from jax import lax
from jax.experimental import pallas as pl
from jax.experimental.pallas import tpu as pltpu
from jax.sharding import PartitionSpec as P

MESH = pl.DeviceIdType.MESH
LANES = 128
VMEM = pl.BlockSpec(memory_space=pltpu.VMEM)
SMEM = pl.BlockSpec(memory_space=pltpu.SMEM)
ANY = pl.BlockSpec(memory_space=pl.ANY)
F32 = jnp.float32
BF16 = jnp.bfloat16


def remote(src, dst, send, recv, grp, dev):
    return pltpu.make_async_remote_copy(
        src_ref=src,
        dst_ref=dst,
        send_sem=send,
        recv_sem=recv,
        device_id=(grp, dev),
        device_id_type=MESH,
    )


def meet(peers):
    barrier = pltpu.get_barrier_semaphore()
    for grp, dev in peers:
        pl.semaphore_signal(barrier, inc=1, device_id=(grp, dev), device_id_type=MESH)
    pl.semaphore_wait(barrier, len(peers))


def slot_of(request, blocks, b, p, capacity, own):
    position = blocks[b, p]
    owner = position // capacity
    return owner * own + request[0, owner, position - owner * capacity]


def flip(index, mask):
    out = index
    bit = 1
    while bit <= mask:
        if mask & bit:
            out = out + bit - 2 * bit * lax.rem(index // bit, 2)
        bit *= 2
    return out


def whole_kernel(
    groups,
    devs,
    request,
    blocks,
    batch_atom,
    stored_any,
    values_any,
    offset_any,
    weight_any,
    exchange_any,
    xyz_any,
    result,
    density,
    table,
    gathered,
    values,
    turned,
    offset,
    weight,
    exchange,
    xyz,
    sums,
    picks,
    part,
    paired,
    sent_1,
    came_1,
    sent_2,
    came_2,
    outgoing,
    arrived,
    across,
    final,
    local_sem,
    gather_sems,
    table_sems,
    wide_sems,
    pair_sems,
    end_sems,
):
    g, me = lax.axis_index("grp"), lax.axis_index("dev")
    own, tile = result.shape[0], result.shape[1]
    slots, capacity = gathered.shape[0], request.shape[2]
    batches, points, width = values.shape
    rel = width // tile
    pairs = batches * rel * rel
    atoms = xyz.shape[1]
    devices = groups * devs
    half, quarter = own // 2, own // 4
    send_a, recv_a, send_y, recv_y, send_b, recv_b = (gather_sems.at[i] for i in range(6))

    mine = pltpu.make_async_copy(
        stored_any, gathered.at[pl.ds(me * own, own)], local_sem.at[0]
    )
    mine.start()
    loads = []
    for i, (source, target) in enumerate(
        (
            (values_any, values),
            (xyz_any, xyz),
            (offset_any, offset),
            (weight_any, weight),
            (exchange_any, exchange),
        )
    ):
        loads.append(pltpu.make_async_copy(source, target, local_sem.at[1 + i]))
        loads[-1].start()
    others = [
        (lax.rem(g + j, groups), lax.rem(me + k, devs))
        for j in range(groups)
        for k in range(devs)
        if j or k
    ]
    meet(others)
    mine.wait()

    first_row = lax.rem(g, 2) * half
    lane_row = first_row + lax.rem(g // 2, 2) * quarter

    def piece(k):
        return gathered.at[pl.ds(flip(me, k) * own + lane_row, quarter)]

    came = {}

    def onward(k):
        came[k + 1] = remote(
            piece(k), piece(k), send_a.at[k + 1], recv_a.at[k + 1], g, flip(me, 1)
        )
        came[k + 1].start()

    onward(0)
    for k in range(2, devs, 2):
        came[k] = remote(piece(0), piece(0), send_a.at[k], recv_a.at[k], g, flip(me, k))
        came[k].start()

    for copy in loads:
        copy.wait()
    lane = lax.broadcasted_iota(jnp.int32, (1, LANES), 1)
    slot_of_pair = [
        slot_of(request, blocks, p // (rel * rel), p % (rel * rel), capacity, own)
        for p in range(pairs)
    ]
    known = jnp.full((1, LANES), -1, jnp.int32)
    for p in range(pairs):
        known = jnp.where(lane == p, slot_of_pair[p], known)
    for p in range(pairs):
        same = known == slot_of_pair[p]
        before = jnp.max(jnp.where(same & (lane < p), lane, -1))
        last = jnp.max(jnp.where(same, lane, -1))
        picks[0, p] = jnp.where(before < 0, 2 * pairs, before)
        picks[1, p] = jnp.where(before < 0, last, before + pairs)
    for s in range(slots):
        last = jnp.max(jnp.where(known == s, lane, -1))
        picks[2, s] = jnp.where(last < 0, 2 * pairs, last + pairs)
    for b in range(batches):
        turned[b] = values[b].T
    sums[2 * pairs] = jnp.zeros((tile, tile), F32)
    spot = lax.broadcasted_iota(jnp.int32, (3, atoms), 1)
    centres = [
        jnp.sum(jnp.where(spot == batch_atom[b], xyz[...], 0.0), axis=1, keepdims=True)
        for b in range(batches)
    ]
    entry = jnp.zeros((1, LANES), F32)
    for b in range(batches):
        for k in range(3):
            entry = jnp.where(lane == b * 8 + 4 + k, centres[b][k : k + 1], entry)
        entry = jnp.where(lane == b * 8 + 7, batch_atom[b].astype(F32), entry)

    order = []
    for k in range(2, devs, 2):
        order += [k, k - 1]
    order.append(devs - 1)
    sideways, passed = {}, []

    def hand_over(k):
        sideways[k].wait_recv()
        rows = pl.ds(flip(me, k) * own + first_row, half)
        copy = remote(
            gathered.at[rows], gathered.at[rows], send_b.at[k], recv_b.at[k], flip(g, 1), me
        )
        copy.start()
        passed.append(copy)

    for step, k in enumerate(order):
        came[k].wait_recv()
        sideways[k] = remote(piece(k), piece(k), send_y.at[k], recv_y.at[k], flip(g, 2), me)
        sideways[k].start()
        if k % 2 == 0:
            onward(k)
        if step >= 2:
            hand_over(order[step - 2])
    for k in order[-2:]:
        hand_over(k)
    pending = list(came.values()) + list(sideways.values()) + passed
    for copy in passed:
        copy.wait_recv()

    for b in range(batches):
        tiles = [
            [
                gathered[slot_of(request, blocks, b, i * rel + j, capacity, own)]
                for j in range(rel)
            ]
            for i in range(rel)
        ]
        matrix = jnp.concatenate([jnp.concatenate(row, axis=1) for row in tiles], axis=0)
        right = jnp.dot(matrix, turned[b], preferred_element_type=F32)
        row = jnp.sum(right * turned[b].astype(F32), axis=0, keepdims=True)
        density[pl.ds(b, 1), :] = row
        weighted = row * weight[pl.ds(b, 1), :]
        moments = [jnp.sum(weighted, axis=1, keepdims=True)]
        for k in range(3):
            moments.append(
                jnp.sum(weighted * offset[k, pl.ds(b, 1), :], axis=1, keepdims=True)
            )
        for k in range(4):
            entry = jnp.where(lane == b * 8 + k, moments[k], entry)
    here = g * devs + me
    table[here] = entry

    spread = []
    for i, (to_g, to_me) in enumerate(others[::-1]):
        copy = remote(
            table.at[here], table.at[here], table_sems.at[0, i], table_sems.at[1, i], to_g, to_me
        )
        copy.start()
        spread.append(copy)

    def accumulate(b, factor, index, base):
        scaled = (turned[b].astype(F32) * factor).astype(BF16)
        term = jnp.dot(scaled, values[b], preferred_element_type=F32)
        for i in range(rel):
            for j in range(rel):
                p = (b * rel + i) * rel + j
                sums[base + p] = (
                    term[i * tile : (i + 1) * tile, j * tile : (j + 1) * tile]
                    + sums[picks[index, p]]
                )

    for b in range(batches):
        pick = pl.ds(b, 1)
        accumulate(b, weight[pick, :] * exchange[pick, :] * density[pick, :], 0, 0)
    places = [
        [centres[b][k : k + 1] + offset[k, pl.ds(b, 1), :] for k in range(3)]
        for b in range(batches)
    ]
    for copy in spread:
        copy.wait_recv()

    chunk = min(devices, 32)

    def gather(step, fields):
        fields = list(fields)
        rows = table[pl.ds(step * chunk, chunk), 0, :]
        for source in range(batches):
            column = [rows[:, source * 8 + k : source * 8 + k + 1] for k in range(7)]
            for b in range(batches):
                gap = [places[b][k] - column[4 + k] for k in range(3)]
                inverse = lax.rsqrt(
                    gap[0] * gap[0] + gap[1] * gap[1] + gap[2] * gap[2] + 1.0
                )
                cube = inverse * inverse * inverse
                dipole = column[1] * gap[0] + column[2] * gap[1] + column[3] * gap[2]
                fields[b] = fields[b] + jnp.sum(
                    column[0] * inverse + dipole * cube, axis=0, keepdims=True
                )
        return tuple(fields)

    fields = tuple(jnp.zeros((1, points), F32) for _ in range(batches))
    if devices == chunk:
        fields = gather(0, fields)
    else:
        fields = lax.fori_loop(0, devices // chunk, gather, fields)
    for b in range(batches):
        accumulate(b, weight[pl.ds(b, 1), :] * fields[b], 1, pairs)
    for copy in pending + spread:
        copy.wait_send()

    quads = groups // 4
    quad, corner = g // 4, lax.rem(g, 4)
    core, side = lax.rem(g, 2), lax.rem(g // 2, 2)
    pair, beside = flip(g, 1), flip(g, 2)
    turn_y, turn_x = 1 - 2 * side, 1 - 2 * lax.rem(me, 2)
    one = (g + (1 - core) * 2 * turn_y, me + core * turn_x)
    two = (g + core * 2 * turn_y, me + (1 - core) * turn_x)

    send_a, recv_a, send_1, recv_1, send_2, recv_2, send_b, recv_b = (
        wide_sems.at[i] for i in range(8)
    )
    send_c, recv_c = pair_sems.at[0], pair_sems.at[1]
    send_d, recv_d = end_sems.at[0], end_sems.at[1]

    def fill(owner, row, count):
        for r in range(count):
            s = owner * own + row + r
            part[s] = sums[picks[2, s]].astype(BF16)

    order = list(range(devs - 1, -1, -1))
    halves, first, second, out = {}, {}, {}, {}
    for k in order:
        fill(flip(me, k), (1 - core) * half, half)
        halves[k] = remote(
            part.at[pl.ds(flip(me, k) * own + (1 - core) * half, half)],
            paired.at[k],
            send_a.at[k],
            recv_a.at[k],
            pair,
            me,
        )
        halves[k].start()

    for k in order:
        fill(flip(me, k), core * half, half)

    def of_pair(a, b, k):
        over_x = core * a + (1 - core) * b
        which = side + ((1 - core) * a + core * b) * turn_y
        row = (flip(me, k) + over_x * turn_x) * own + core * half + which * quarter
        here = part[pl.ds(row, quarter)]
        there = paired[k + over_x, pl.ds(which * quarter, quarter)]
        return here.astype(F32) + there.astype(F32)

    def of_four(b, k):
        first[k + b].wait_recv()
        return of_pair(0, b, k) + came_1[k + b].astype(F32)

    def of_eight(k):
        second[k].wait_recv()
        return of_four(0, k) + came_2[k // 2].astype(F32)

    def step_1(k):
        halves[k + 1].wait_recv()
        halves[k].wait_recv()
        for b in (1, 0):
            slot = k + b
            sent_1[slot] = of_pair(1, b, k).astype(BF16)
            first[slot] = remote(
                sent_1.at[slot], came_1.at[slot], send_1.at[slot], recv_1.at[slot], *one
            )
            first[slot].start()

    def step_2(k):
        slot = k // 2
        sent_2[slot] = of_four(1, k).astype(BF16)
        second[k] = remote(
            sent_2.at[slot], came_2.at[slot], send_2.at[slot], recv_2.at[slot], *two
        )
        second[k].start()

    def step_3(k):
        slot = k // 2
        outgoing[slot] = of_eight(k).astype(BF16)
        out[k] = remote(
            outgoing.at[slot],
            arrived.at[slot],
            send_b.at[slot],
            recv_b.at[slot],
            g,
            flip(me, k),
        )
        out[k].start()

    planes = list(range(devs - 2, -1, -2))
    for step, k in enumerate(planes):
        step_1(k)
        if step >= 1:
            step_2(planes[step - 1])
        if step >= 2:
            step_3(planes[step - 2])
    step_2(0)
    for k in planes[-2:-1]:
        step_3(k)
    whole = of_eight(0)
    for k in planes[:-1]:
        out[k].wait_recv()
        whole = whole + arrived[k // 2].astype(F32)
    late = []
    if quads > 1:
        across[quad] = whole.astype(BF16)
        for j in range(1, quads):
            copy = remote(
                across.at[quad],
                across.at[quad],
                send_c.at[j],
                recv_c.at[j],
                lax.rem(quad + j, quads) * 4 + corner,
                me,
            )
            copy.start()
            late.append(copy)
        for copy in late:
            copy.wait_recv()
        whole = across[0].astype(F32)
        for j in range(1, quads):
            whole = whole + across[j].astype(F32)
    part_rows = pl.ds(core * half + side * quarter, quarter)
    half_rows = pl.ds(core * half, half)
    final[part_rows] = whole.astype(BF16)
    for step, (where, to) in enumerate(((part_rows, beside), (half_rows, pair))):
        copy = remote(
            final.at[where], final.at[where], send_d.at[step], recv_d.at[step], to, me
        )
        copy.start()
        copy.wait_recv()
        late.append(copy)
    for copy in [*halves.values(), *first.values(), *second.values(), *out.values(), *late]:
        copy.wait_send()
    result[...] = final[...]


def finish_kernel(batches, hamiltonian, density, table, result, density_out, multipoles):
    result[...] = hamiltonian[...]
    density_out[...] = density[...]
    devices, atoms = table.shape[0], multipoles.shape[1]
    chunk = min(devices, 32)
    spot = lax.broadcasted_iota(jnp.int32, (1, atoms), 1).astype(F32)

    def gather(step, moments):
        moments = list(moments)
        rows = table[pl.ds(step * chunk, chunk), 0, :]
        for source in range(batches):
            hit = rows[:, source * 8 + 7 : source * 8 + 8] == spot
            for k in range(4):
                column = rows[:, source * 8 + k : source * 8 + k + 1]
                moments[k] = moments[k] + jnp.sum(
                    jnp.where(hit, column, 0.0), axis=0, keepdims=True
                )
        return tuple(moments)

    moments = tuple(jnp.zeros((1, atoms), F32) for _ in range(4))
    if devices == chunk:
        moments = gather(0, moments)
    else:
        moments = lax.fori_loop(0, devices // chunk, gather, moments)
    for k in range(4):
        multipoles[pl.ds(k, 1), :] = moments[k]


def on_device(
    groups,
    devs,
    basis_values,
    stored_density_blocks,
    device_request,
    batch_blocks,
    batch_atom,
    point_offset,
    point_weight,
    exchange_kernel,
    atom_xyz,
):
    batches, points, width = basis_values.shape
    own, tile = stored_density_blocks.shape[:2]
    slots = devs * own
    atoms = atom_xyz.shape[1]
    devices = groups * devs
    half, quarter = own // 2, own // 4
    pairs = batches * (width // tile) ** 2
    dma = pltpu.SemaphoreType.DMA

    hamiltonian, density, table = pl.pallas_call(
        functools.partial(whole_kernel, groups, devs),
        out_shape=(
            pltpu.VMEM((own, tile, tile), BF16),
            pltpu.VMEM((batches, points), F32),
            pltpu.VMEM((devices, 1, LANES), F32),
        ),
        in_specs=[SMEM, SMEM, SMEM, ANY, ANY, ANY, ANY, ANY, ANY],
        out_specs=(VMEM, VMEM, VMEM),
        scratch_shapes=[
            pltpu.VMEM((slots, tile, tile), BF16),
            pltpu.VMEM((batches, points, width), BF16),
            pltpu.VMEM((batches, width, points), BF16),
            pltpu.VMEM(point_offset.shape, F32),
            pltpu.VMEM((batches, points), F32),
            pltpu.VMEM((batches, points), F32),
            pltpu.VMEM(atom_xyz.shape, F32),
            pltpu.VMEM((2 * pairs + 1, tile, tile), F32),
            pltpu.SMEM((3, max(slots, pairs)), jnp.int32),
            pltpu.VMEM((slots, tile, tile), BF16),
            pltpu.VMEM((devs, half, tile, tile), BF16),
            pltpu.VMEM((devs, quarter, tile, tile), BF16),
            pltpu.VMEM((devs, quarter, tile, tile), BF16),
            pltpu.VMEM((devs // 2, quarter, tile, tile), BF16),
            pltpu.VMEM((devs // 2, quarter, tile, tile), BF16),
            pltpu.VMEM((devs // 2, quarter, tile, tile), BF16),
            pltpu.VMEM((devs // 2, quarter, tile, tile), BF16),
            pltpu.VMEM((groups // 4, quarter, tile, tile), BF16),
            pltpu.VMEM((own, tile, tile), BF16),
            dma((6,)),
            dma((6, devs)),
            dma((2, devices)),
            dma((8, devs)),
            dma((2, groups // 4)),
            dma((2, 2)),
        ],
        compiler_params=pltpu.CompilerParams(collective_id=0, has_side_effects=True),
    )(
        device_request,
        batch_blocks,
        batch_atom,
        stored_density_blocks,
        basis_values,
        point_offset,
        point_weight,
        exchange_kernel,
        atom_xyz,
    )

    return pl.pallas_call(
        functools.partial(finish_kernel, batches),
        out_shape=(
            jax.ShapeDtypeStruct((own, tile, tile), BF16),
            jax.ShapeDtypeStruct((batches, points), F32),
            jax.ShapeDtypeStruct((4, atoms), F32),
        ),
        in_specs=[VMEM, VMEM, VMEM],
        out_specs=(VMEM, VMEM, VMEM),
    )(hamiltonian, density, table)


def solution(mesh):
    return jax.shard_map(
        functools.partial(on_device, mesh.shape["grp"], mesh.shape["dev"]),
        mesh=mesh,
        in_specs=(
            P(("grp", "dev"), None, None),
            P("dev", None, None),
            P(("grp", "dev"), None, None),
            P(("grp", "dev"), None),
            P(("grp", "dev")),
            P(None, ("grp", "dev"), None),
            P(("grp", "dev"), None),
            P(("grp", "dev"), None),
            P(),
        ),
        out_specs=(P("dev", None, None), P(("grp", "dev"), None), P()),
        check_vma=False,
    )
```
